32 devices in a mesh: dom: 8 (over y, x, core), sub: 4 (over z).
Axes of the slice: x: 2, y: 2, z: 4, core: 2. Of those that a mesh axis runs over, the one named last changes fastest.
Arguments:
- features: bfloat16 [32768, 602], P(('dom', 'sub')), may hold values from -6 to 6
- w_inner: bfloat16 [602, 256], replicated, may hold values from -0.25 to 0.25
- bias_inner: float32 [256], replicated, may hold values from -6 to 6
- w_outer: bfloat16 [256, 41], replicated, may hold values from -0.375 to 0.375
- bias_outer: float32 [41], replicated, may hold values from -6 to 6
- tiles: bfloat16 [256, 32, 128, 128], P(('dom', 'sub')), may hold values from -3 to 3
- tile_col: int32 [256, 32], P(('dom', 'sub')), may hold values from 0 to 39, as said below
- degrees: int32 [32768], P(('dom', 'sub')), may hold values from 1 to 32
- send_rows: int32 [32, 32, 128], P(('dom', 'sub')), may hold values from -1 to 1023, as said below
Outputs:
- logits: float32 [32768, 41], P(('dom', 'sub'))
The draws below stay inside these ranges and needn't reach their ends.
Inputs may be any that keep to these rules, and one draw needn't show every extreme that they name: send_rows[e, p, s] is the row, among device e's 1024 vertices, that fills slot s of e's list for device p, or -1 for an unused slot; live slots come first and every list has 1 to 128 live slots; every sender has a full list, and in every draw some device receives full lists from all senders. tile_col[d * 8 + r, t] is the column block, in device d's column space, of tile t of row block r; the 32 column blocks of a row block are distinct.
All inputs are finite; a program needn't handle non-finite values.
Results may differ from the reference program's by a relative error of at most 0.0042.
Values may be sent and summed in bfloat16 or wider, within the bound.
A program may use at most 128 MiB of HBM per device.

```python
import jax
import jax.numpy as jnp
from jax import lax

F_IN = 602
HID = 256
CLASSES = 41
BLK = 128
TILES = 32
V_DEV = 1024
PEERS = 32
ROW_BLOCKS = 8
COL_BLOCKS = 40
VERTS = 32768


def draw_send_rows(key, part):
    key_rows = jax.random.fold_in(key, 11)
    key_counts = jax.random.fold_in(key, 12)
    key_full = jax.random.fold_in(key, 13)
    key_target = jax.random.fold_in(key, 14)
    picked = jax.random.randint(key_rows, (PEERS, PEERS, BLK), 0, V_DEV)
    counts = jax.random.randint(key_counts, (PEERS, PEERS), 1, BLK + 1)
    full_peer = jax.random.randint(key_full, (PEERS,), 0, PEERS)
    target = jax.random.randint(key_target, (), 0, PEERS)
    peer_ids = jnp.arange(PEERS)
    counts = jnp.where(peer_ids[None, :] == full_peer[:, None], BLK, counts)
    counts = jnp.where(peer_ids[None, :] == target, BLK, counts)
    slots = jnp.arange(BLK)
    return jnp.where(slots[None, None, :] < counts[:, :, None], picked, -1).astype(jnp.int32)


def draw_tile_col(key, part):
    keys = jax.random.split(jax.random.fold_in(key, 21), PEERS)
    orders = jax.vmap(lambda single: jax.random.permutation(single, COL_BLOCKS))(keys)
    flat = jnp.arange(ROW_BLOCKS * TILES) % COL_BLOCKS
    picked = orders[:, flat]
    return picked.reshape(PEERS * ROW_BLOCKS, TILES).astype(jnp.int32)


def place_ends(drawn, stream_key, least, top_value):
    index_at = [jax.random.randint(jax.random.fold_in(stream_key, axis), (), 0, length) for axis, length in enumerate(drawn.shape)]
    main_axis = drawn.shape.index(max(drawn.shape))
    beside = index_at[:main_axis] + [(index_at[main_axis] + 1) % drawn.shape[main_axis]] + index_at[main_axis + 1:]
    return drawn.at[tuple(index_at)].set(least).at[tuple(beside)].set(top_value)


def levels(rng, dims, shards, low, largest):
    def one(position, blocks):
        draws = jax.random.uniform(jax.random.fold_in(jax.random.fold_in(rng, 6), position), (blocks,), jnp.float32, low / len(shards), largest / len(shards))
        return jnp.repeat(jnp.exp(draws), dims[position] // blocks).reshape((-1,) + (1,) * (len(dims) - position - 1))

    gain = one(*shards[0])
    for cut in shards[1:]:
        gain = gain * one(*cut)
    return gain


def centred(stream_key, extent, scale, reach, cuts=(), kind=jnp.bfloat16):
    drawn = scale * jax.random.normal(stream_key, extent, jnp.float32)
    if cuts:
        drawn = drawn * levels(stream_key, extent, cuts, -0.22, 0.18)
    return jnp.clip(drawn, -reach, reach).astype(kind)


def setup_inputs(seed: int = 0) -> dict:
    key_of = jax.random.split(jax.random.key(seed), 10)
    return {
        "features": centred(key_of[0], (VERTS, F_IN), 1.0, 6.0, ((0, 32),)),
        "w_inner": centred(key_of[1], (F_IN, HID), F_IN ** -0.5, 0.25),
        "bias_inner": centred(key_of[2], (HID,), 1.0, 6.0, (), jnp.float32),
        "w_outer": centred(key_of[3], (HID, CLASSES), HID ** -0.5, 0.375),
        "bias_outer": centred(key_of[4], (CLASSES,), 1.0, 6.0, (), jnp.float32),
        "tiles": centred(key_of[5], (PEERS * ROW_BLOCKS, TILES, BLK, BLK), (12.0 / (TILES * BLK) ** 0.5), 3.0, ((0, 32),)),
        "tile_col": draw_tile_col(jax.random.fold_in(key_of[9], 71), 0),
        "degrees": place_ends(jax.random.randint(key_of[7], (VERTS,), 1, 33), jax.random.fold_in(key_of[7], 1), 1, 32).astype(jnp.int32),
        "send_rows": draw_send_rows(jax.random.fold_in(key_of[9], 71), 0),
    }


def aggregate(feature_rows, tiles, tile_col, send_rows):
    width = feature_rows.shape[1]
    by_device = feature_rows.reshape(PEERS, V_DEV, width)
    tile_sets = tiles.reshape(PEERS, ROW_BLOCKS, TILES, BLK, BLK)
    col_sets = tile_col.reshape(PEERS, ROW_BLOCKS, TILES)

    def per_target(target):
        slot_rows = lax.dynamic_index_in_dim(send_rows, target, 1, keepdims=False)
        clipped = jnp.clip(slot_rows, 0, V_DEV - 1).astype(jnp.int32)
        fetched = jnp.take_along_axis(by_device, clipped[:, :, None], axis=1)
        fetched = jnp.where((slot_rows >= 0)[:, :, None], fetched, jnp.zeros((), feature_rows.dtype))
        own_rows = lax.dynamic_index_in_dim(by_device, target, 0, keepdims=False)
        columns = jnp.concatenate([own_rows.reshape(ROW_BLOCKS, BLK, width), fetched], axis=0)
        target_tiles = lax.dynamic_index_in_dim(tile_sets, target, 0, keepdims=False)
        target_cols = lax.dynamic_index_in_dim(col_sets, target, 0, keepdims=False)
        blocks = columns[target_cols]
        summed = jnp.einsum('rtij,rtjw->riw', target_tiles.astype(jnp.float32), blocks.astype(jnp.float32))
        return summed.reshape(V_DEV, width)
    results = lax.map(per_target, jnp.arange(PEERS, dtype=jnp.int32))
    return results.reshape(PEERS * V_DEV, width)

def reference(features, w_inner, bias_inner, w_outer, bias_outer, tiles, tile_col, degrees, send_rows):
    inv_sqrt = lax.rsqrt(degrees.astype(jnp.float32))[:, None]
    projected = (jnp.dot(features, w_inner, preferred_element_type=jnp.float32) * inv_sqrt).astype(jnp.bfloat16)
    agg_inner = aggregate(projected, tiles, tile_col, send_rows)
    hidden = (inv_sqrt * jax.nn.relu(inv_sqrt * agg_inner + bias_inner)).astype(jnp.bfloat16)
    scores = jnp.dot(hidden, w_outer, preferred_element_type=jnp.float32).astype(jnp.bfloat16)
    agg_outer = aggregate(scores, tiles, tile_col, send_rows)
    return inv_sqrt * agg_outer + bias_outer
```

```python
import functools

import jax
import jax.numpy as jnp
from jax import lax
from jax.experimental import pallas as pl
from jax.experimental.pallas import tpu as pltpu
from jax.sharding import PartitionSpec as P

MESH = pl.DeviceIdType.MESH
NT = (((1,), (1,)), ((), ()))


def kernel(
    n_dom, n_sub, ft, w_inner, bias, w_outer, degrees, lists, where_tile, tiles_hbm, out,
    proj, out_in, got_in, acc_in, w_pad, scores, out_sc, got_sc, acc_sc, tiles,
    tile_sem, send_in, recv_in, send_sc, recv_sc,
):
    dom, sub = lax.axis_index("dom"), lax.axis_index("sub")
    peers = n_dom * n_sub
    hid, verts = proj.shape
    rows, per_row, blk, _ = tiles.shape
    own = verts // blk
    classes = w_outer.shape[0]

    def flip(a):
        total, bit = 0, 1
        while bit < n_dom:
            total = total + lax.rem(lax.div(dom, bit) + lax.div(a, bit), 2) * bit
            bit *= 2
        return total

    def target(k):
        return flip(lax.div(k, n_sub)), lax.rem(sub + lax.rem(k, n_sub), n_sub)

    def source(k):
        return flip(lax.div(k, n_sub)) * n_sub + lax.rem(sub + n_sub - lax.rem(k, n_sub), n_sub)

    def copy(src, dst, sends, recvs, k):
        return pltpu.make_async_remote_copy(
            src_ref=src.at[k], dst_ref=dst.at[k], send_sem=sends.at[k], recv_sem=recvs.at[k],
            device_id=target(k), device_id_type=MESH,
        )

    barrier = pltpu.get_barrier_semaphore()

    @pl.loop(1, peers)
    def _(k):
        pl.semaphore_signal(barrier, inc=1, device_id=target(k), device_id_type=MESH)

    tile_copy = pltpu.make_async_copy(tiles_hbm, tiles, tile_sem)
    tile_copy.start()
    inv = lax.rsqrt(degrees[...].astype(jnp.float32))
    w_t = w_inner[...].T
    wide = 2 * blk
    for v in range(0, verts, wide):
        part = jnp.dot(w_t, ft[:, v:v + wide], preferred_element_type=jnp.float32)
        proj[:, v:v + wide] = (part * inv[:, v:v + wide]).astype(proj.dtype)
    pl.semaphore_wait(barrier, peers - 1)

    def pick(k, table):
        slot_rows = []
        for each in (k, k + 1):
            to_dom, to_sub = target(each)
            slot_rows.append(lists[pl.ds(to_dom * n_sub + to_sub, 1), :])
        slots = jnp.concatenate(slot_rows, axis=1)
        hot = lax.broadcasted_iota(jnp.int32, (verts, 2 * blk), 0) == slots
        hot = jnp.where(hot, 1.0, 0.0).astype(table.dtype)
        return jnp.dot(table[...], hot, preferred_element_type=jnp.float32).astype(table.dtype)

    def deliver(table, outgoing, got, sends, recvs):
        first = pick(0, table)
        got[0] = first[:, :blk]
        outgoing[1] = first[:, blk:]
        copy(outgoing, got, sends, recvs, 1).start()

        @pl.loop(1, peers // 2)
        def _(pair):
            k = 2 * pair
            picked = pick(k, table)
            outgoing[k] = picked[:, :blk]
            outgoing[k + 1] = picked[:, blk:]
            copy(outgoing, got, sends, recvs, k).start()
            copy(outgoing, got, sends, recvs, k + 1).start()

    def add(acc, block, c0, c1, fresh):
        def tile(r, c):
            t = where_tile[r, c]
            found = tiles[r, jnp.maximum(t, 0)]
            return jnp.where(t >= 0, found, jnp.zeros_like(found))

        for r in range(0, rows, 2):
            weights = jnp.concatenate(
                [jnp.concatenate([tile(r + q, c0), tile(r + q, c1)], axis=1) for q in range(2)],
                axis=0,
            )
            term = lax.dot_general(block, weights, NT, preferred_element_type=jnp.float32)
            span = slice(r * blk, (r + 2) * blk)
            acc[:, span] = term if fresh else acc[:, span] + term

    def aggregate(table, outgoing, got, sends, recvs, acc):
        for c in range(0, own, 2):
            add(acc, table[:, c * blk:(c + 2) * blk], c, c + 1, c == 0)

        def arrived(k):
            block = jnp.concatenate([got[k], got[k + 1]], axis=1)
            add(acc, block, own + source(k), own + source(k + 1), False)

        copy(outgoing, got, sends, recvs, 1).wait_recv()
        arrived(0)

        @pl.loop(1, peers // 2)
        def _(pair):
            k = 2 * pair
            copy(outgoing, got, sends, recvs, k).wait_recv()
            copy(outgoing, got, sends, recvs, k + 1).wait_recv()
            arrived(k)

    deliver(proj, out_in, got_in, send_in, recv_in)
    w_pad[...] = jnp.zeros_like(w_pad)
    w_pad[0:classes, :] = w_outer[...]
    bias_col = jnp.broadcast_to(bias[...], (blk, hid)).T
    tile_copy.wait()
    aggregate(proj, out_in, got_in, send_in, recv_in, acc_in)
    for v in range(0, verts, blk):
        span = slice(v, v + blk)
        scale = inv[:, span]
        hidden = scale * jnp.maximum(scale * acc_in[:, span] + bias_col, 0.0)
        scores[:, span] = jnp.dot(
            w_pad[...], hidden.astype(jnp.bfloat16), preferred_element_type=jnp.float32
        ).astype(scores.dtype)
    deliver(scores, out_sc, got_sc, send_sc, recv_sc)
    aggregate(scores, out_sc, got_sc, send_sc, recv_sc, acc_sc)
    out[...] = acc_sc[0:classes, :]

    @pl.loop(1, peers)
    def _(k):
        copy(out_in, got_in, send_in, recv_in, k).wait_send()
        copy(out_sc, got_sc, send_sc, recv_sc, k).wait_send()


def on_device(
    n_dom, n_sub,
    features, w_inner, bias_inner, w_outer, bias_outer, tiles, tile_col, degrees, send_rows
):
    peers = n_dom * n_sub
    verts, hid = features.shape[0], w_inner.shape[1]
    classes = w_outer.shape[1]
    padded = 16 * ((classes + 15) // 16)
    blk = tiles.shape[2]
    columns = verts // blk + peers
    order = jnp.arange(tiles.shape[1], dtype=jnp.int32)
    hit = tile_col[:, None, :] == jnp.arange(columns, dtype=jnp.int32)[None, :, None]
    where_tile = jnp.max(jnp.where(hit, order, -1), axis=2)
    vmem = pl.BlockSpec(memory_space=pltpu.VMEM)
    bf16, f32 = jnp.bfloat16, jnp.float32
    agg = pl.pallas_call(
        functools.partial(kernel, n_dom, n_sub),
        out_shape=jax.ShapeDtypeStruct((classes, verts), f32),
        in_specs=[vmem] * 6
        + [pl.BlockSpec(memory_space=pltpu.SMEM), pl.BlockSpec(memory_space=pl.ANY)],
        out_specs=vmem,
        scratch_shapes=[
            pltpu.VMEM((hid, verts), bf16),
            pltpu.VMEM((peers, hid, blk), bf16),
            pltpu.VMEM((peers, hid, blk), bf16),
            pltpu.VMEM((hid, verts), f32),
            pltpu.VMEM((padded, hid), bf16),
            pltpu.VMEM((padded, verts), bf16),
            pltpu.VMEM((peers, padded, blk), bf16),
            pltpu.VMEM((peers, padded, blk), bf16),
            pltpu.VMEM((padded, verts), f32),
            pltpu.VMEM(tiles.shape, bf16),
            pltpu.SemaphoreType.DMA,
            pltpu.SemaphoreType.DMA((peers,)),
            pltpu.SemaphoreType.DMA((peers,)),
            pltpu.SemaphoreType.DMA((peers,)),
            pltpu.SemaphoreType.DMA((peers,)),
        ],
        compiler_params=pltpu.CompilerParams(
            collective_id=0, has_side_effects=True, vmem_limit_bytes=56 * 1024 * 1024
        ),
    )(
        features.T, w_inner, bias_inner[None, :], w_outer.T, degrees[None, :], send_rows[0],
        where_tile, tiles,
    )
    inv_sqrt = lax.rsqrt(degrees.astype(f32))[:, None]
    return inv_sqrt * agg.T + bias_outer


def solution(mesh):
    return jax.shard_map(
        functools.partial(on_device, mesh.shape["dom"], mesh.shape["sub"]),
        mesh=mesh,
        in_specs=(
            P(("dom", "sub"), None),
            P(),
            P(),
            P(),
            P(),
            P(("dom", "sub"), None, None, None),
            P(("dom", "sub"), None),
            P(("dom", "sub")),
            P(("dom", "sub"), None, None),
        ),
        out_specs=P(("dom", "sub"), None),
        check_vma=False,
    )
```

```python
import functools

import jax
import jax.numpy as jnp
from jax import lax
from jax.experimental import pallas as pl
from jax.experimental.pallas import tpu as pltpu
from jax.sharding import PartitionSpec as P

MESH = pl.DeviceIdType.MESH
NT = (((1,), (1,)), ((), ()))


def kernel(
    n_dom, n_sub, ft, w_inner, bias, w_outer, degrees, lists, where_tile, tiles_hbm, out,
    proj, out_in, got_in, acc_in, w_pad, scores, out_sc, got_sc, acc_sc, tiles,
    tile_sem, send_in, recv_in, send_sc, recv_sc,
    far_proj=None, far_lists=None, proj_send=None, proj_recv=None, lists_send=None, lists_recv=None,
):
    dom, sub = lax.axis_index("dom"), lax.axis_index("sub")
    peers = n_dom * n_sub
    hid, verts = proj.shape
    rows, per_row, blk, _ = tiles.shape
    own = verts // blk
    classes = w_outer.shape[0]

    def flip(a):
        total, bit = 0, 1
        while bit < n_dom:
            total = total + lax.rem(lax.div(dom, bit) + lax.div(a, bit), 2) * bit
            bit *= 2
        return total

    def target(k):
        return flip(lax.div(k, n_sub)), lax.rem(sub + lax.rem(k, n_sub), n_sub)

    def source(k):
        return flip(lax.div(k, n_sub)) * n_sub + lax.rem(sub + n_sub - lax.rem(k, n_sub), n_sub)

    def copy(src, dst, sends, recvs, k):
        return pltpu.make_async_remote_copy(
            src_ref=src.at[k], dst_ref=dst.at[k], send_sem=sends.at[k], recv_sem=recvs.at[k],
            device_id=target(k), device_id_type=MESH,
        )

    barrier = pltpu.get_barrier_semaphore()

    @pl.loop(1, peers)
    def _(k):
        pl.semaphore_signal(barrier, inc=1, device_id=target(k), device_id_type=MESH)

    tile_copy = pltpu.make_async_copy(tiles_hbm, tiles, tile_sem)
    tile_copy.start()
    inv = lax.rsqrt(degrees[...].astype(jnp.float32))
    w_t = w_inner[...].T
    wide = 2 * blk
    for v in range(0, verts, wide):
        part = jnp.dot(w_t, ft[:, v:v + wide], preferred_element_type=jnp.float32)
        proj[:, v:v + wide] = (part * inv[:, v:v + wide]).astype(proj.dtype)
    pl.semaphore_wait(barrier, peers - 1)

    def pick_for(first, second, table, lists):
        slots = jnp.concatenate([lists[pl.ds(first, 1), :], lists[pl.ds(second, 1), :]], axis=1)
        hot = lax.broadcasted_iota(jnp.int32, (verts, 2 * blk), 0) == slots
        hot = jnp.where(hot, 1.0, 0.0).astype(table.dtype)
        return jnp.dot(table[...], hot, preferred_element_type=jnp.float32).astype(table.dtype)

    def pick(k, table):
        index = [to_dom * n_sub + to_sub for to_dom, to_sub in (target(k), target(k + 1))]
        return pick_for(*index, table, lists)

    def deliver(table, outgoing, got, sends, recvs):
        first = pick(0, table)
        got[0] = first[:, :blk]
        outgoing[1] = first[:, blk:]
        copy(outgoing, got, sends, recvs, 1).start()

        @pl.loop(1, peers // 2)
        def _(pair):
            k = 2 * pair
            picked = pick(k, table)
            outgoing[k] = picked[:, :blk]
            outgoing[k + 1] = picked[:, blk:]
            copy(outgoing, got, sends, recvs, k).start()
            copy(outgoing, got, sends, recvs, k + 1).start()

    def add(acc, block, c0, c1, fresh):
        def tile(r, c):
            t = where_tile[r, c]
            found = tiles[r, jnp.maximum(t, 0)]
            return jnp.where(t >= 0, found, jnp.zeros_like(found))

        for r in range(0, rows, 2):
            weights = jnp.concatenate(
                [jnp.concatenate([tile(r + q, c0), tile(r + q, c1)], axis=1) for q in range(2)],
                axis=0,
            )
            term = lax.dot_general(block, weights, NT, preferred_element_type=jnp.float32)
            span = slice(r * blk, (r + 2) * blk)
            acc[:, span] = term if fresh else acc[:, span] + term

    def add_own(table, acc):
        for c in range(0, own, 2):
            add(acc, table[:, c * blk:(c + 2) * blk], c, c + 1, c == 0)

    def aggregate(table, outgoing, got, sends, recvs, acc):
        add_own(table, acc)

        def arrived(k):
            block = jnp.concatenate([got[k], got[k + 1]], axis=1)
            add(acc, block, own + source(k), own + source(k + 1), False)

        copy(outgoing, got, sends, recvs, 1).wait_recv()
        arrived(0)

        @pl.loop(1, peers // 2)
        def _(pair):
            k = 2 * pair
            copy(outgoing, got, sends, recvs, k).wait_recv()
            copy(outgoing, got, sends, recvs, k + 1).wait_recv()
            arrived(k)

    relay = far_proj is not None
    if relay:
        half = lax.div(sub, 2)
        sibling, near, far = 1 + 4 * half - sub, 2 - half, 3 - 3 * half
        middle = sub == 1 + half
        mine = dom * n_sub + sub
        per_step = 2 * n_dom

        def to_slot(j, source_index, to_dom, to_sub):
            return pltpu.make_async_remote_copy(
                src_ref=out_in.at[j], dst_ref=got_in.at[source_index], send_sem=send_in.at[j],
                recv_sem=recv_in.at[source_index], device_id=(to_dom, to_sub), device_id_type=MESH,
            )

        def block_copies(slot):
            return [
                pltpu.make_async_remote_copy(
                    src_ref=src, dst_ref=dst.at[slot], send_sem=sent, recv_sem=came.at[slot],
                    device_id=(dom, near), device_id_type=MESH,
                )
                for src, dst, sent, came in (
                    (proj, far_proj, proj_send, proj_recv), (lists, far_lists, lists_send, lists_recv)
                )
            ]

        def send_block(slot):
            for each in block_copies(slot):
                each.start()

        def hand_out(table, lists, source_index, base):
            def picked_for(a):
                row = flip(a) * n_sub
                return pick_for(row + sub, row + sibling, table, lists)

            first = picked_for(0)
            got_in[source_index] = first[:, :blk]
            out_in[base + 1] = first[:, blk:]
            to_slot(base + 1, source_index, dom, sibling).start()

            @pl.loop(1, n_dom)
            def _(a):
                picked = picked_for(a)
                j = base + 2 * a
                out_in[j] = picked[:, :blk]
                out_in[j + 1] = picked[:, blk:]
                to_slot(j + 1, source_index, flip(a), sibling).start()
                to_slot(j, source_index, flip(a), sub).start()

        def relay_block(slot, from_sub):
            for each in block_copies(slot):
                each.wait_recv()
            hand_out(
                far_proj.at[slot], far_lists.at[slot], dom * n_sub + from_sub, (slot + 1) * per_step
            )

        def wait_for(index):
            to_slot(0, index, dom, sibling).wait_recv()

        def add_pair(e0, e1):
            block = jnp.concatenate([got_in[e0], got_in[e1]], axis=1)
            add(acc_in, block, own + e0, own + e1, False)

        pl.when(middle)(lambda: send_block(0))
        hand_out(proj, lists, mine, 0)
        pl.when(jnp.logical_not(middle))(lambda: send_block(1))
    else:
        deliver(proj, out_in, got_in, send_in, recv_in)
    w_pad[...] = jnp.zeros_like(w_pad)
    w_pad[0:classes, :] = w_outer[...]
    bias_col = jnp.broadcast_to(bias[...], (blk, hid)).T
    tile_copy.wait()
    if relay:
        add_own(proj, acc_in)
        pl.when(middle)(lambda: relay_block(0, near))
        wait_for(dom * n_sub + sibling)
        add_pair(mine, dom * n_sub + sibling)

        @pl.loop(1, n_dom)
        def _(a):
            row = flip(a) * n_sub
            wait_for(row + sub)
            wait_for(row + sibling)
            add_pair(row + sub, row + sibling)

        pl.when(middle)(lambda: relay_block(1, far))
        for plane in (near, far):
            @pl.when(jnp.logical_not(middle))
            def _():
                wait_for(dom * n_sub + plane)

            wait_for(flip(1) * n_sub + plane)
            add_pair(dom * n_sub + plane, flip(1) * n_sub + plane)

            @pl.loop(1, n_dom // 2)
            def _(pair):
                e0, e1 = flip(2 * pair) * n_sub + plane, flip(2 * pair + 1) * n_sub + plane
                wait_for(e0)
                wait_for(e1)
                add_pair(e0, e1)
    else:
        aggregate(proj, out_in, got_in, send_in, recv_in, acc_in)
    for v in range(0, verts, blk):
        span = slice(v, v + blk)
        scale = inv[:, span]
        hidden = scale * jnp.maximum(scale * acc_in[:, span] + bias_col, 0.0)
        scores[:, span] = jnp.dot(
            w_pad[...], hidden.astype(jnp.bfloat16), preferred_element_type=jnp.float32
        ).astype(scores.dtype)
    deliver(scores, out_sc, got_sc, send_sc, recv_sc)
    aggregate(scores, out_sc, got_sc, send_sc, recv_sc, acc_sc)
    out[...] = acc_sc[0:classes, :]

    @pl.loop(1, peers)
    def _(k):
        copy(out_sc, got_sc, send_sc, recv_sc, k).wait_send()

    if relay:
        for each in block_copies(0):
            each.wait_send()

        @pl.loop(1, per_step)
        def _(j):
            to_slot(j, 0, dom, sibling).wait_send()

        @pl.when(middle)
        def _():
            @pl.loop(1, per_step)
            def _(j):
                to_slot(per_step + j, 0, dom, sibling).wait_send()
                to_slot(2 * per_step + j, 0, dom, sibling).wait_send()
    else:
        @pl.loop(1, peers)
        def _(k):
            copy(out_in, got_in, send_in, recv_in, k).wait_send()


def on_device(
    n_dom, n_sub,
    features, w_inner, bias_inner, w_outer, bias_outer, tiles, tile_col, degrees, send_rows
):
    peers = n_dom * n_sub
    verts, hid = features.shape[0], w_inner.shape[1]
    classes = w_outer.shape[1]
    padded = 16 * ((classes + 15) // 16)
    blk = tiles.shape[2]
    columns = verts // blk + peers
    order = jnp.arange(tiles.shape[1], dtype=jnp.int32)
    hit = tile_col[:, None, :] == jnp.arange(columns, dtype=jnp.int32)[None, :, None]
    where_tile = jnp.max(jnp.where(hit, order, -1), axis=2)
    relay = n_sub == 4
    lists_out = 6 * n_dom if relay else peers
    vmem = pl.BlockSpec(memory_space=pltpu.VMEM)
    bf16, f32 = jnp.bfloat16, jnp.float32
    agg = pl.pallas_call(
        functools.partial(kernel, n_dom, n_sub),
        out_shape=jax.ShapeDtypeStruct((classes, verts), f32),
        in_specs=[vmem] * 6
        + [pl.BlockSpec(memory_space=pltpu.SMEM), pl.BlockSpec(memory_space=pl.ANY)],
        out_specs=vmem,
        scratch_shapes=[
            pltpu.VMEM((hid, verts), bf16),
            pltpu.VMEM((lists_out, hid, blk), bf16),
            pltpu.VMEM((peers, hid, blk), bf16),
            pltpu.VMEM((hid, verts), f32),
            pltpu.VMEM((padded, hid), bf16),
            pltpu.VMEM((padded, verts), bf16),
            pltpu.VMEM((peers, padded, blk), bf16),
            pltpu.VMEM((peers, padded, blk), bf16),
            pltpu.VMEM((padded, verts), f32),
            pltpu.VMEM(tiles.shape, bf16),
            pltpu.SemaphoreType.DMA,
            pltpu.SemaphoreType.DMA((lists_out,)),
            pltpu.SemaphoreType.DMA((peers,)),
            pltpu.SemaphoreType.DMA((peers,)),
            pltpu.SemaphoreType.DMA((peers,)),
        ]
        + (
            [
                pltpu.VMEM((2, hid, verts), bf16),
                pltpu.VMEM((2, peers, blk), jnp.int32),
                pltpu.SemaphoreType.DMA,
                pltpu.SemaphoreType.DMA((2,)),
                pltpu.SemaphoreType.DMA,
                pltpu.SemaphoreType.DMA((2,)),
            ]
            if relay
            else []
        ),
        compiler_params=pltpu.CompilerParams(
            collective_id=0, has_side_effects=True, vmem_limit_bytes=56 * 1024 * 1024
        ),
    )(
        features.T, w_inner, bias_inner[None, :], w_outer.T, degrees[None, :], send_rows[0],
        where_tile, tiles,
    )
    inv_sqrt = lax.rsqrt(degrees.astype(f32))[:, None]
    return inv_sqrt * agg.T + bias_outer


def solution(mesh):
    return jax.shard_map(
        functools.partial(on_device, mesh.shape["dom"], mesh.shape["sub"]),
        mesh=mesh,
        in_specs=(
            P(("dom", "sub"), None),
            P(),
            P(),
            P(),
            P(),
            P(("dom", "sub"), None, None, None),
            P(("dom", "sub"), None),
            P(("dom", "sub")),
            P(("dom", "sub"), None, None),
        ),
        out_specs=P(("dom", "sub"), None),
        check_vma=False,
    )
```

```python
import functools

import jax
import jax.numpy as jnp
from jax import lax
from jax.experimental import pallas as pl
from jax.experimental.pallas import tpu as pltpu
from jax.sharding import PartitionSpec as P

MESH = pl.DeviceIdType.MESH
NT = (((1,), (1,)), ((), ()))


def kernel(
    n_dom, n_sub, *refs,
):
    hbm, (tiles_hbm, out), staged, refs = refs[:7], refs[7:9], refs[9:16], refs[16:]
    run(n_dom, n_sub, hbm, staged, tiles_hbm, out, *refs)


def run(
    n_dom, n_sub, hbm, staged, tiles_hbm, out, stage_sem, found, where_tile, found_sem,
    proj, out_in, got_in, acc_in, w_pad, scores, out_sc, got_sc, acc_sc, tiles,
    tile_sem, send_in, recv_in, send_sc, recv_sc,
    far_proj=None, far_lists=None, proj_send=None, proj_recv=None, lists_send=None, lists_recv=None,
):
    ft, w_inner, bias, w_outer, degrees, lists, tile_col = staged
    dom, sub = lax.axis_index("dom"), lax.axis_index("sub")
    peers = n_dom * n_sub
    hid, verts = proj.shape
    rows, per_row, blk, _ = tiles.shape
    own = verts // blk
    classes = w_outer.shape[0]

    def flip(a):
        total, bit = 0, 1
        while bit < n_dom:
            total = total + lax.rem(lax.div(dom, bit) + lax.div(a, bit), 2) * bit
            bit *= 2
        return total

    def target(k):
        return flip(lax.div(k, n_sub)), lax.rem(sub + lax.rem(k, n_sub), n_sub)

    def source(k):
        return flip(lax.div(k, n_sub)) * n_sub + lax.rem(sub + n_sub - lax.rem(k, n_sub), n_sub)

    def copy(src, dst, sends, recvs, k):
        return pltpu.make_async_remote_copy(
            src_ref=src.at[k], dst_ref=dst.at[k], send_sem=sends.at[k], recv_sem=recvs.at[k],
            device_id=target(k), device_id_type=MESH,
        )

    barrier = pltpu.get_barrier_semaphore()

    @pl.loop(1, peers)
    def _(k):
        pl.semaphore_signal(barrier, inc=1, device_id=target(k), device_id_type=MESH)

    staging = [
        pltpu.make_async_copy(src, dst, stage_sem.at[i]) for i, (src, dst) in enumerate(zip(hbm, staged))
    ]
    for each in staging:
        each.start()
    tile_copy = pltpu.make_async_copy(tiles_hbm, tiles, tile_sem)
    tile_copy.start()
    for each in staging:
        each.wait()
    inv = lax.rsqrt(degrees[...].astype(jnp.float32))
    w_t = w_inner[...].T
    wide = 2 * blk
    for v in range(0, verts, wide):
        part = jnp.dot(w_t, ft[:, v:v + wide], preferred_element_type=jnp.float32)
        proj[:, v:v + wide] = (part * inv[:, v:v + wide]).astype(proj.dtype)
    cols = tile_col[...]
    lane = lax.broadcasted_iota(jnp.int32, found.shape, 1)
    place = jnp.full(found.shape, -1, jnp.int32)
    for t in range(per_row):
        place = jnp.where(cols[:, t:t + 1] == lane, t, place)
    found[...] = place
    found_copy = pltpu.make_async_copy(found, where_tile, found_sem)
    found_copy.start()
    pl.semaphore_wait(barrier, peers - 1)

    def pick_for(first, second, table, lists):
        slots = jnp.concatenate([lists[pl.ds(first, 1), :], lists[pl.ds(second, 1), :]], axis=1)
        hot = lax.broadcasted_iota(jnp.int32, (verts, 2 * blk), 0) == slots
        hot = jnp.where(hot, 1.0, 0.0).astype(table.dtype)
        return jnp.dot(table[...], hot, preferred_element_type=jnp.float32).astype(table.dtype)

    def pick(k, table):
        index = [to_dom * n_sub + to_sub for to_dom, to_sub in (target(k), target(k + 1))]
        return pick_for(*index, table, lists)

    def deliver(table, outgoing, got, sends, recvs):
        first = pick(0, table)
        got[0] = first[:, :blk]
        outgoing[1] = first[:, blk:]
        copy(outgoing, got, sends, recvs, 1).start()

        @pl.loop(1, peers // 2)
        def _(pair):
            k = 2 * pair
            picked = pick(k, table)
            outgoing[k] = picked[:, :blk]
            outgoing[k + 1] = picked[:, blk:]
            copy(outgoing, got, sends, recvs, k).start()
            copy(outgoing, got, sends, recvs, k + 1).start()

    def add(acc, block, c0, c1, fresh):
        def tile(r, c):
            t = where_tile[r, c]
            found = tiles[r, jnp.maximum(t, 0)]
            return jnp.where(t >= 0, found, jnp.zeros_like(found))

        for r in range(0, rows, 2):
            weights = jnp.concatenate(
                [jnp.concatenate([tile(r + q, c0), tile(r + q, c1)], axis=1) for q in range(2)],
                axis=0,
            )
            term = lax.dot_general(block, weights, NT, preferred_element_type=jnp.float32)
            span = slice(r * blk, (r + 2) * blk)
            acc[:, span] = term if fresh else acc[:, span] + term

    def add_own(table, acc):
        for c in range(0, own, 2):
            add(acc, table[:, c * blk:(c + 2) * blk], c, c + 1, c == 0)

    def aggregate(table, outgoing, got, sends, recvs, acc):
        add_own(table, acc)

        def arrived(k):
            block = jnp.concatenate([got[k], got[k + 1]], axis=1)
            add(acc, block, own + source(k), own + source(k + 1), False)

        copy(outgoing, got, sends, recvs, 1).wait_recv()
        arrived(0)

        @pl.loop(1, peers // 2)
        def _(pair):
            k = 2 * pair
            copy(outgoing, got, sends, recvs, k).wait_recv()
            copy(outgoing, got, sends, recvs, k + 1).wait_recv()
            arrived(k)

    relay = far_proj is not None
    if relay:
        half = lax.div(sub, 2)
        sibling, near, far = 1 + 4 * half - sub, 2 - half, 3 - 3 * half
        middle = sub == 1 + half
        mine = dom * n_sub + sub
        per_step = 2 * n_dom
        direct = 2

        def to_slot(j, source_index, to_dom, to_sub):
            return pltpu.make_async_remote_copy(
                src_ref=out_in.at[j], dst_ref=got_in.at[source_index], send_sem=send_in.at[j],
                recv_sem=recv_in.at[source_index], device_id=(to_dom, to_sub), device_id_type=MESH,
            )

        def block_copies(slot):
            return [
                pltpu.make_async_remote_copy(
                    src_ref=src, dst_ref=dst.at[slot], send_sem=sent, recv_sem=came.at[slot],
                    device_id=(dom, near), device_id_type=MESH,
                )
                for src, dst, sent, came in (
                    (proj, far_proj, proj_send, proj_recv), (lists, far_lists, lists_send, lists_recv)
                )
            ]

        def send_block(slot):
            for each in block_copies(slot):
                each.start()

        def hand_out(table, lists, source_index, base, skip):
            def picked_for(a):
                row = flip(a) * n_sub
                return pick_for(row + sub, row + sibling, table, lists)

            first = picked_for(0)
            got_in[source_index] = first[:, :blk]
            if skip == 0:
                out_in[base + 1] = first[:, blk:]
                to_slot(base + 1, source_index, dom, sibling).start()
            for a in range(1, skip):
                out_in[base + 2 * a] = picked_for(a)[:, :blk]
                to_slot(base + 2 * a, source_index, flip(a), sub).start()

            @pl.loop(max(1, skip), n_dom)
            def _(a):
                picked = picked_for(a)
                j = base + 2 * a
                out_in[j] = picked[:, :blk]
                out_in[j + 1] = picked[:, blk:]
                to_slot(j + 1, source_index, flip(a), sibling).start()
                to_slot(j, source_index, flip(a), sub).start()

        def relay_block(slot, from_sub):
            for each in block_copies(slot):
                each.wait_recv()
            hand_out(
                far_proj.at[slot], far_lists.at[slot], dom * n_sub + from_sub, (slot + 1) * per_step,
                direct,
            )

        def send_direct():
            rows_for = [flip(a) * n_sub + far for a in range(2)]
            picked = pick_for(*rows_for, proj, lists)
            for a in range(2):
                j = per_step + 2 * a + 1
                out_in[j] = picked[:, a * blk:(a + 1) * blk]
                to_slot(j, mine, flip(a), far).start()

        def wait_for(index):
            to_slot(0, index, dom, sibling).wait_recv()

        def add_pair(e0, e1):
            block = jnp.concatenate([got_in[e0], got_in[e1]], axis=1)
            add(acc_in, block, own + e0, own + e1, False)

        pl.when(middle)(lambda: send_block(0))
        hand_out(proj, lists, mine, 0, 0)
        pl.when(jnp.logical_not(middle))(lambda: send_block(1))
        send_direct()
    else:
        deliver(proj, out_in, got_in, send_in, recv_in)
    w_pad[...] = jnp.zeros_like(w_pad)
    w_pad[0:classes, :] = w_outer[...]
    bias_col = jnp.broadcast_to(bias[...], (blk, hid)).T
    tile_copy.wait()
    found_copy.wait()
    if relay:
        add_own(proj, acc_in)
        pl.when(middle)(lambda: relay_block(0, near))
        wait_for(dom * n_sub + sibling)
        add_pair(mine, dom * n_sub + sibling)

        @pl.loop(1, n_dom)
        def _(a):
            row = flip(a) * n_sub
            wait_for(row + sub)
            wait_for(row + sibling)
            add_pair(row + sub, row + sibling)

        pl.when(middle)(lambda: relay_block(1, far))
        for plane in (near, far):
            @pl.when(jnp.logical_not(middle))
            def _():
                wait_for(dom * n_sub + plane)

            wait_for(flip(1) * n_sub + plane)
            add_pair(dom * n_sub + plane, flip(1) * n_sub + plane)

            @pl.loop(1, n_dom // 2)
            def _(pair):
                e0, e1 = flip(2 * pair) * n_sub + plane, flip(2 * pair + 1) * n_sub + plane
                wait_for(e0)
                wait_for(e1)
                add_pair(e0, e1)
    else:
        aggregate(proj, out_in, got_in, send_in, recv_in, acc_in)
    for v in range(0, verts, blk):
        span = slice(v, v + blk)
        scale = inv[:, span]
        hidden = scale * jnp.maximum(scale * acc_in[:, span] + bias_col, 0.0)
        scores[:, span] = jnp.dot(
            w_pad[...], hidden.astype(jnp.bfloat16), preferred_element_type=jnp.float32
        ).astype(scores.dtype)
    deliver(scores, out_sc, got_sc, send_sc, recv_sc)
    aggregate(scores, out_sc, got_sc, send_sc, recv_sc, acc_sc)
    out[...] = acc_sc[0:classes, :]

    @pl.loop(1, peers)
    def _(k):
        copy(out_sc, got_sc, send_sc, recv_sc, k).wait_send()

    if relay:
        for each in block_copies(0):
            each.wait_send()

        @pl.loop(1, per_step)
        def _(j):
            to_slot(j, 0, dom, sibling).wait_send()

        for a in range(direct):
            to_slot(per_step + 2 * a + 1, 0, dom, sibling).wait_send()

        @pl.when(middle)
        def _():
            for base in (per_step, 2 * per_step):
                for a in range(1, direct):
                    to_slot(base + 2 * a, 0, dom, sibling).wait_send()

            @pl.loop(2 * direct, per_step)
            def _(j):
                to_slot(per_step + j, 0, dom, sibling).wait_send()
                to_slot(2 * per_step + j, 0, dom, sibling).wait_send()
    else:
        @pl.loop(1, peers)
        def _(k):
            copy(out_in, got_in, send_in, recv_in, k).wait_send()


def on_device(
    n_dom, n_sub,
    features, w_inner, bias_inner, w_outer, bias_outer, tiles, tile_col, degrees, send_rows
):
    peers = n_dom * n_sub
    verts, hid = features.shape[0], w_inner.shape[1]
    classes = w_outer.shape[1]
    padded = 16 * ((classes + 15) // 16)
    blk = tiles.shape[2]
    columns = verts // blk + peers
    lanes = 128 * ((columns + 127) // 128)
    small = (
        features.T, w_inner, bias_inner[None, :], w_outer.T, degrees[None, :], send_rows[0], tile_col
    )
    relay = n_sub == 4
    lists_out = 6 * n_dom if relay else peers
    vmem = pl.BlockSpec(memory_space=pltpu.VMEM)
    bf16, f32 = jnp.bfloat16, jnp.float32
    agg = pl.pallas_call(
        functools.partial(kernel, n_dom, n_sub),
        out_shape=jax.ShapeDtypeStruct((classes, verts), f32),
        in_specs=[pl.BlockSpec(memory_space=pl.ANY)] * 8,
        out_specs=vmem,
        scratch_shapes=[pltpu.VMEM(each.shape, each.dtype) for each in small]
        + [
            pltpu.SemaphoreType.DMA((7,)),
            pltpu.VMEM((tiles.shape[0], lanes), jnp.int32),
            pltpu.SMEM((tiles.shape[0], lanes), jnp.int32),
            pltpu.SemaphoreType.DMA,
            pltpu.VMEM((hid, verts), bf16),
            pltpu.VMEM((lists_out, hid, blk), bf16),
            pltpu.VMEM((peers, hid, blk), bf16),
            pltpu.VMEM((hid, verts), f32),
            pltpu.VMEM((padded, hid), bf16),
            pltpu.VMEM((padded, verts), bf16),
            pltpu.VMEM((peers, padded, blk), bf16),
            pltpu.VMEM((peers, padded, blk), bf16),
            pltpu.VMEM((padded, verts), f32),
            pltpu.VMEM(tiles.shape, bf16),
            pltpu.SemaphoreType.DMA,
            pltpu.SemaphoreType.DMA((lists_out,)),
            pltpu.SemaphoreType.DMA((peers,)),
            pltpu.SemaphoreType.DMA((peers,)),
            pltpu.SemaphoreType.DMA((peers,)),
        ]
        + (
            [
                pltpu.VMEM((2, hid, verts), bf16),
                pltpu.VMEM((2, peers, blk), jnp.int32),
                pltpu.SemaphoreType.DMA,
                pltpu.SemaphoreType.DMA((2,)),
                pltpu.SemaphoreType.DMA,
                pltpu.SemaphoreType.DMA((2,)),
            ]
            if relay
            else []
        ),
        compiler_params=pltpu.CompilerParams(
            collective_id=0, has_side_effects=True, vmem_limit_bytes=56 * 1024 * 1024
        ),
    )(*small, tiles)
    inv_sqrt = lax.rsqrt(degrees.astype(f32))[:, None]
    return inv_sqrt * agg.T + bias_outer


def solution(mesh):
    return jax.shard_map(
        functools.partial(on_device, mesh.shape["dom"], mesh.shape["sub"]),
        mesh=mesh,
        in_specs=(
            P(("dom", "sub"), None),
            P(),
            P(),
            P(),
            P(),
            P(("dom", "sub"), None, None, None),
            P(("dom", "sub"), None),
            P(("dom", "sub")),
            P(("dom", "sub"), None, None),
        ),
        out_specs=P(("dom", "sub"), None),
        check_vma=False,
    )
```
